256 devices in a mesh: rep: 2 (over y), ep: 16 (over z), tp: 8 (over x, core).
Axes of the slice: x: 4, y: 2, z: 16, core: 2. Of those that a mesh axis runs over, the one named last changes fastest.
The devices are a block of a 4x16x16 slice.
Arguments:
- residual_in: bfloat16 [4096, 4096], P(('rep', 'ep'), 'tp'), parts along dimension 0, may hold values from -3.2 to 3.2
- queries: bfloat16 [4096, 4096], P(('rep', 'ep'), 'tp'), parts along dimension 0, may hold values from -120 to 120
- key_rows: bfloat16 [4096, 256], P(('rep', 'ep')), parts along dimension 0, may hold values from -4 to 4
- value_rows: bfloat16 [4096, 256], P(('rep', 'ep')), parts along dimension 0, may hold values from -6 to 6
- seq_lengths: int32 [32], P(('rep', 'ep')), parts along dimension 0, may hold values from 64 to 128
- out_weight: bfloat16 [4096, 4096], P('tp', 'ep'), may hold values from -0.09375 to 0.09375
- norm_gain: float32 [4096], P('tp'), may hold values from 0.25 to 1.75
- expert_ids: int32 [4096, 8], P(('rep', 'ep')), parts along dimension 0, may hold values from 0 to 31, all different within a row; in each aligned block of 128 rows (0 to 127, 128 to 255, ...) at most 48 rows name the same one
- gate_probs: float32 [4096, 8], P(('rep', 'ep')), parts along dimension 0, may hold values from 0.03 to 0.5
- gate_weight: bfloat16 [32, 4096, 1536], P('ep', None, 'tp'), may hold values from -0.09375 to 0.09375
- up_weight: bfloat16 [32, 4096, 1536], P('ep', None, 'tp'), may hold values from -0.09375 to 0.09375
- down_weight: bfloat16 [32, 1536, 4096], P('ep', None, 'tp'), may hold values from -0.15625 to 0.15625
Outputs:
- layer_out: bfloat16 [4096, 4096], P(('rep', 'ep'), 'tp'), parts along dimension 0
The draws below stay inside these ranges and needn't reach their ends.
There are 2 independent parts, one for each index of `rep`. The reference program is written for one: setup_inputs(seed, part) draws one part's arguments, and reference() takes and returns one part's arrays. A program takes and returns all parts, laid end to end along the dimension named above; an argument that names none is the same for every part. Nothing has to cross between parts.
Inputs may be any that keep to these rules, and one draw needn't show every extreme that they name: `expert_ids`: each row names 8 different experts. Within the rows of one sequence no expert is named by more than 48 rows, a bound that some block reaches. `seq_lengths`: each sequence's number of valid tokens.
All inputs are finite; a program needn't handle non-finite values.
Results may differ from the reference program's by a relative error of at most 0.015.
Values may be sent and summed in bfloat16 or wider, within the bound.
No kernel may reach another device: no remote copies, remote signals or barrier semaphores. Data moves between devices by JAX's collectives and lax.ppermute only.
A program may use at most 128 MiB of HBM per device.

```python
import math
import jax
import jax.numpy as jnp
import numpy as np
from jax import lax

D = 4096
HEADS = 32
KV_HEADS = 2
HEAD_DIM = 128
FF = 1536
TOP = 8
SEQ = 128
EXPERTS = 32
TOKENS = 2048
CAP = 48
N_EP = 16


def base_keys(key):
    raw = jax.random.normal(jax.random.fold_in(key, 71), (TOKENS, KV_HEADS * HEAD_DIM), jnp.float32)
    return jnp.clip(raw, -4.0, 4.0)


def draw_key_rows(key, part):
    keys_wide = base_keys(key)
    return keys_wide.astype(jnp.bfloat16)


def draw_queries(key, part):
    raw = jax.random.normal(jax.random.fold_in(key, 72), (TOKENS, HEADS * HEAD_DIM), jnp.float32)
    result = jnp.clip(raw, -4.0, 4.0)
    return result.astype(jnp.bfloat16)


def draw_residual_in(key, part):
    column_scale = 0.4 + 0.8 * jnp.arange(D, dtype=jnp.float32) / D
    values = jnp.clip(jax.random.normal(jax.random.fold_in(key, 81), (TOKENS, D), jnp.float32), -4.0, 4.0)
    return (0.5 * values * column_scale[None, :]).astype(jnp.bfloat16)


def with_ends(values, rng, smallest, high):
    shape = values.shape
    spot = [jax.random.randint(jax.random.fold_in(rng, axis), (), 0, shape[axis]) for axis in range(len(shape))]
    values = values.at[tuple(spot)].set(smallest)
    longest = shape.index(max(shape))
    spot[longest] = (spot[longest] + 1) % shape[longest]
    return values.at[tuple(spot)].set(high)


def shard_levels(key, shape, shards, smallest, top_value):
    loudness = 1.0
    for dim, shards_of in shards:
        steps = jax.random.uniform(jax.random.fold_in(jax.random.fold_in(key, 6), dim), (shards_of,), jnp.float32, smallest / len(shards), top_value / len(shards))
        loudness = loudness * jnp.repeat(jnp.exp(steps), shape[dim] // shards_of).reshape((-1,) + (1,) * (len(shape) - 1 - dim))
    return loudness


def routed_block(stream_key, own, number, rows, number_of, top, most, skew):
    ranking = jax.random.permutation(stream_key, number_of)
    crowded, common = portions_of(number_of, rows * top, most, skew, True), portions_of(number_of, rows * top, most, skew, False)
    places = jnp.arange(number_of)

    def named(sizes, offset_by):
        used = int((sizes > 0).sum())
        fixed = max(1, used // 4)
        passed = fixed + (places - fixed + offset_by * (used - fixed)) % max(1, number_of - fixed)
        return jnp.zeros((number_of,), jnp.int32).at[ranking[jnp.where(places < fixed, places, passed)]].set(jnp.asarray(sizes, jnp.int32))

    sizes = jnp.where(number % 4 == 0, named(crowded, number // 4), named(common, number - number // 4 - 1))
    mixed = jax.random.permutation(jax.random.fold_in(own, 3), number_of)
    giver, sink = mixed[0:number_of // 2 * 2:2], mixed[1:number_of // 2 * 2:2]
    slack = jnp.minimum(sizes[giver] - 1, most - sizes[sink]) // 2
    slack = jnp.where((giver == ranking[0]) | (sink == ranking[0]) | (sizes[sink] == 0), 0, jnp.maximum(slack, 0))
    passed = jax.random.randint(jax.random.fold_in(own, 4), (number_of // 2,), 0, 1 << 20) % (slack + 1)
    sizes = sizes.at[giver].add(-passed).at[sink].add(passed)
    members = jnp.searchsorted(jnp.cumsum(sizes), jnp.arange(rows * top), side="right").astype(jnp.int32)
    table = members.reshape(top, rows).T
    table = table[jax.random.permutation(jax.random.fold_in(own, 1), rows)]
    offset_by = jax.random.randint(jax.random.fold_in(own, 2), (rows, 1), 0, top)
    return jnp.take_along_axis(table, (jnp.arange(top)[None, :] + offset_by) % top, axis=1)


def portions_of(amount, total, bound, lean, full):
    loads = [(1 << 20) // math.isqrt(grade ** lean) + 1 for grade in range(1, amount + 1)]
    largest = bound if full else min(bound, max(-(-total // amount), total * loads[0] // sum(loads)))
    least = 1 if total - largest >= amount - 1 else 0
    given, rest = [largest] + [least] * (amount - 1), total - largest - least * (amount - 1)
    while rest > 0:
        free = [i for i in range(1, amount) if given[i] < largest] or [i for i in range(1, amount) if given[i] < bound]
        whole, left = sum([loads[i] for i in free]), rest
        for i in free:
            addition = min(bound - given[i], max(1, left * loads[i] // whole), rest)
            given[i] = given[i] + addition
            rest = rest - addition
    return np.array(given)


def gaussian(own_key, dims, spread, most, pieces=(), kind=jnp.bfloat16):
    drawn = spread * jax.random.normal(own_key, dims, jnp.float32)
    if pieces:
        drawn = drawn * shard_levels(own_key, dims, pieces, -0.22, 0.18)
    return jnp.clip(drawn, -most, most).astype(kind)


def setup_inputs(seed: int = 0, part: int = 0) -> dict:
    keys = jax.random.split(jax.random.key(seed), 13)
    part_keys = jax.random.split(jax.random.fold_in(keys[12], part), 13)
    residual_in = draw_residual_in(jax.random.fold_in(jax.random.fold_in(keys[12], part), 71), part)
    queries = draw_queries(jax.random.fold_in(jax.random.fold_in(keys[12], part), 71), part)
    key_rows = draw_key_rows(jax.random.fold_in(jax.random.fold_in(keys[12], part), 71), part)
    value_rows = gaussian(part_keys[3], (TOKENS, KV_HEADS * HEAD_DIM), 1.0, 6.0, ((0, 16),))
    seq_lengths = with_ends(jax.random.randint(part_keys[4], (N_EP,), SEQ // 2, SEQ + 1), jax.random.fold_in(part_keys[4], 1), SEQ // 2, SEQ).astype(jnp.int32)
    out_weight = gaussian(keys[5], (HEADS * HEAD_DIM, D), (HEADS * HEAD_DIM) ** -0.5, 0.09375, ((0, 8), (1, 16)))
    norm_gain = jnp.clip(1.0 + 0.15 * jax.random.normal(keys[6], (D,), jnp.float32), 0.25, 1.75)
    expert_ids_keys = jax.random.split(jax.random.fold_in(part_keys[7], 1), TOKENS // SEQ)
    expert_ids_turns = jax.random.permutation(jax.random.fold_in(part_keys[7], 3), TOKENS // SEQ)
    expert_ids = jax.vmap(lambda own, number: routed_block(jax.random.fold_in(part_keys[7], 2), own, number, SEQ, EXPERTS, TOP, CAP, 1))(expert_ids_keys, expert_ids_turns).reshape((TOKENS, TOP))
    gate_probs = jnp.clip(jnp.exp(math.log(0.5) - 2.8134107 * jax.random.uniform(part_keys[8], (TOKENS, TOP), jnp.float32) ** shard_levels(part_keys[8], (TOKENS, TOP), ((0, 16),), -0.2, 0.2)), 0.03, 0.5)
    gate_weight = gaussian(keys[9], (EXPERTS, D, FF), D ** -0.5, 0.09375, ((0, 16), (2, 8)))
    up_weight = gaussian(keys[10], (EXPERTS, D, FF), D ** -0.5, 0.09375, ((0, 16), (2, 8)))
    down_weight = gaussian(keys[11], (EXPERTS, FF, D), FF ** -0.5, 0.15625, ((0, 16), (2, 8)))
    return dict(residual_in=residual_in, queries=queries, key_rows=key_rows, value_rows=value_rows, seq_lengths=seq_lengths, out_weight=out_weight, norm_gain=norm_gain, expert_ids=expert_ids, gate_probs=gate_probs, gate_weight=gate_weight, up_weight=up_weight, down_weight=down_weight)


EPSILON = 1e-06

def attention_all(queries, key_rows, value_rows, seq_lengths):
    group_size = HEADS // KV_HEADS
    query_four = queries.reshape(N_EP, SEQ, HEADS, HEAD_DIM).astype(jnp.float32)
    key_four = key_rows.reshape(N_EP, SEQ, KV_HEADS, HEAD_DIM).astype(jnp.float32)
    value_four = value_rows.reshape(N_EP, SEQ, KV_HEADS, HEAD_DIM).astype(jnp.float32)
    key_heads = jnp.repeat(key_four, group_size, axis=2)
    value_heads = jnp.repeat(value_four, group_size, axis=2)
    scores = jnp.einsum('bqhd,bkhd->bhqk', query_four, key_heads) * HEAD_DIM ** (-0.5)
    positions = jnp.arange(SEQ, dtype=jnp.int32)
    causal = positions[None, :] <= positions[:, None]
    inside = positions[None, None, :] < seq_lengths[:, None, None]
    visible = causal[None, :, :] & inside
    scores = jnp.where(visible[:, None, :, :], scores, jnp.float32(-1e+30))
    row_peak = lax.optimization_barrier(jnp.max(scores, axis=3, keepdims=True))
    exponent = jnp.exp(scores - row_peak)
    weights = (exponent / lax.optimization_barrier(jnp.sum(exponent, axis=3, keepdims=True))).astype(jnp.bfloat16)
    combined = jnp.einsum('bhqk,bkhd->bqhd', weights.astype(jnp.float32), value_heads)
    return combined.astype(jnp.bfloat16).reshape(TOKENS, HEADS * HEAD_DIM)

def expert_apply(operands):
    rows_in, gate_mat, up_mat, down_mat = operands
    gate_val = jnp.dot(rows_in, gate_mat, preferred_element_type=jnp.float32)
    up_val = jnp.dot(rows_in, up_mat, preferred_element_type=jnp.float32)
    hidden_act = (jax.nn.silu(gate_val) * up_val).astype(jnp.bfloat16)
    return jnp.dot(hidden_act, down_mat, preferred_element_type=jnp.float32)

def reference(residual_in, queries, key_rows, value_rows, seq_lengths, out_weight, norm_gain, expert_ids, gate_probs, gate_weight, up_weight, down_weight):
    attended = attention_all(queries, key_rows, value_rows, seq_lengths)
    attn_proj = jnp.dot(attended, out_weight, preferred_element_type=jnp.float32)
    residual = (residual_in.astype(jnp.float32) + attn_proj).astype(jnp.bfloat16)
    residual_wide = residual.astype(jnp.float32)
    mean_square = lax.optimization_barrier(jnp.sum(residual_wide * residual_wide, axis=1)) / D
    normed = (residual_wide * lax.rsqrt(mean_square + EPSILON)[:, None] * norm_gain).astype(jnp.bfloat16)
    block_ids = expert_ids.reshape(N_EP, SEQ * TOP).astype(jnp.int32)
    one_hot = (block_ids[:, :, None] == jnp.arange(EXPERTS, dtype=jnp.int32)[None, None, :]).astype(jnp.int32)
    earlier = jnp.cumsum(one_hot, axis=1) - one_hot
    slot_rank = lax.optimization_barrier(jnp.sum(earlier * one_hot, axis=2))
    block_index = jnp.arange(N_EP, dtype=jnp.int32)[:, None]
    target = ((block_ids * N_EP + block_index) * CAP + slot_rank).reshape(-1).astype(jnp.int32)
    pair_token = (block_index * SEQ + jnp.arange(SEQ * TOP, dtype=jnp.int32)[None, :] // TOP).reshape(-1).astype(jnp.int32)
    token_of = jnp.zeros((EXPERTS * N_EP * CAP,), jnp.int32).at[target].set(pair_token)
    filled = jnp.zeros((EXPERTS * N_EP * CAP,), jnp.bool_).at[target].set(True)
    taken = jnp.where(filled[:, None], jnp.take(normed, token_of, axis=0), jnp.zeros((), jnp.bfloat16))
    taken = taken.reshape(EXPERTS, N_EP * CAP, D)
    produced = lax.map(expert_apply, (taken, gate_weight, up_weight, down_weight))
    picked = jnp.take(produced.reshape(EXPERTS * N_EP * CAP, D), target, axis=0).reshape(TOKENS, TOP, D)
    mixture = jnp.einsum('tk,tkd->td', gate_probs.astype(jnp.float32), picked, precision=lax.Precision.HIGHEST)
    return (residual_wide + mixture).astype(jnp.bfloat16)
```

```python
import jax
import jax.numpy as jnp
from jax import lax
from jax.sharding import PartitionSpec as P

HEAD_DIM = 128
KV_HEADS = 2
EPSILON = 1e-06
BF = jnp.bfloat16
F32 = jnp.float32


def sent(x, axis, shift):
    n = lax.axis_size(axis)
    return lax.ppermute(x, axis, [(i, (i + shift) % n) for i in range(n)])


def attend(queries, key_rows, value_rows, seq_lengths):
    seq_rows = queries.shape[0]
    heads_here = queries.shape[1] // HEAD_DIM
    group_size = heads_here * lax.axis_size("tp") // KV_HEADS
    kv_column = lax.axis_index("tp") * heads_here // group_size * HEAD_DIM
    key_head = lax.dynamic_slice_in_dim(key_rows, kv_column, HEAD_DIM, 1)
    value_head = lax.dynamic_slice_in_dim(value_rows, kv_column, HEAD_DIM, 1)
    query_three = queries.reshape(seq_rows, heads_here, HEAD_DIM)
    scores = jnp.einsum(
        "qhd,kd->hqk", query_three, key_head, preferred_element_type=F32
    ) * HEAD_DIM ** (-0.5)
    positions = jnp.arange(seq_rows, dtype=jnp.int32)
    visible = (positions[None, :] <= positions[:, None]) & (positions[None, :] < seq_lengths[0])
    scores = jnp.where(visible[None, :, :], scores, F32(-1e30))
    row_peak = jnp.max(scores, axis=2, keepdims=True)
    exponent = jnp.exp(scores - row_peak)
    weights = (exponent / jnp.sum(exponent, axis=2, keepdims=True)).astype(BF)
    combined = jnp.einsum("hqk,kd->qhd", weights, value_head, preferred_element_type=F32)
    return combined.astype(BF).reshape(seq_rows, heads_here * HEAD_DIM)


def near_columns(out_weight):
    ep = lax.axis_size("ep")
    odd = lax.axis_index("ep") % 2
    mate = lax.ppermute(out_weight, "ep", [(i, i ^ 1) for i in range(ep)])
    ahead = sent(out_weight, "ep", -2)
    ahead_mate = lax.ppermute(out_weight, "ep", [(i ^ 1, (i - 2) % ep) for i in range(ep)])
    pair = [jnp.where(odd == 0, a, b) for a, b in
            ((out_weight, mate), (mate, out_weight), (ahead, ahead_mate), (ahead_mate, ahead))]
    return jnp.concatenate(pair, axis=1)


def project(attended, columns):
    ep, tp = lax.axis_size("ep"), lax.axis_size("tp")
    rows, step = attended.shape[0], ep // 4
    tokens = jnp.concatenate(
        [attended, sent(attended, "ep", -step), sent(attended, "ep", -2 * step), sent(attended, "ep", step)],
        axis=0,
    )
    partial = jnp.dot(tokens, columns, preferred_element_type=F32).astype(BF)
    blocks = jnp.moveaxis(partial.reshape(4, rows, 2, -1), 2, 1).reshape(tp, rows, -1)
    arrived = lax.all_to_all(blocks, "tp", split_axis=0, concat_axis=0, tiled=True)
    total = arrived.astype(F32).sum(axis=0).astype(BF)
    owner = []
    for e in range(ep):
        for t in range(tp):
            e_to, t_to = (e + step * (t // 2)) % ep, (e // 2 + t % 2) % tp
            owner.append((e * tp + t, e_to * tp + t_to))
    return lax.ppermute(total, ("ep", "tp"), owner)


def ring_gathered(x, axis):
    n = lax.axis_size(axis)
    found = {0: x}
    up = down = x
    for k in range(1, n // 2 + 1):
        up = sent(up, axis, 1)
        found[-k % n] = up
        if k < n // 2:
            down = sent(down, axis, -1)
            found[k] = down
    return [found[k] for k in range(n)]


def shards(
    residual_in,
    queries,
    key_rows,
    value_rows,
    seq_lengths,
    out_weight,
    norm_gain,
    expert_ids,
    gate_probs,
    gate_weight,
    up_weight,
    down_weight,
):
    rows, width = residual_in.shape
    ep, tp = lax.axis_size("ep"), lax.axis_size("tp")
    e, t = lax.axis_index("ep"), lax.axis_index("tp")
    chip, core = t // 2, t % 2
    local, _, units = gate_weight.shape
    experts = local * ep
    top = expert_ids.shape[1]
    capacity = min(rows, 3 * rows * top // (2 * experts))
    mine = chip % 2
    other = 1 - mine

    columns = near_columns(out_weight)

    def slices(which):
        return jnp.concatenate(
            [lax.dynamic_index_in_dim(w, which, 0, keepdims=False) for w in (gate_weight, up_weight)], axis=1
        )

    kept = slices(mine)
    swapped = lax.ppermute(
        slices(other), "tp", [(i, (i + (2 if i % 2 else -2)) % tp) for i in range(tp)]
    )

    wanted = expert_ids[:, :, None] == jnp.arange(experts, dtype=jnp.int32)[None, None, :]
    chosen = jnp.where(
        wanted.any(axis=1), jnp.where(wanted, gate_probs[:, :, None], 0.0).sum(axis=1), -1.0
    )
    plan = lax.all_to_all(
        chosen.T.reshape(ep, local, rows), "ep", split_axis=0, concat_axis=0, tiled=True
    )

    attended = attend(queries, key_rows, value_rows, seq_lengths)
    head_total = project(attended, columns)
    residual = (residual_in.astype(F32) + head_total.astype(F32)).astype(BF)
    residual_wide = residual.astype(F32)
    square_sum = jnp.sum(residual_wide * residual_wide, axis=1)
    square_all = lax.all_to_all(
        jnp.broadcast_to(square_sum[None, None], (tp, 1, rows)), "tp", 0, 0, tiled=True
    )
    mean_square = square_all.sum(axis=(0, 1)) / (width * tp)
    normed = (residual_wide * lax.rsqrt(mean_square + EPSILON)[:, None] * norm_gain).astype(BF)

    plan = lax.dynamic_slice_in_dim(jnp.concatenate([plan, plan], axis=0), e, ep, 0)
    hit = plan >= 0
    before = jnp.tril(jnp.ones((rows, rows), BF), -1)
    rank = jnp.einsum("sjt,ut->sju", hit.astype(BF), before, preferred_element_type=F32)
    slot = jnp.arange(capacity, dtype=F32)
    pick = (rank[:, :, None, :] == slot[None, None, :, None]) & hit[:, :, None, :]
    picker = pick.astype(BF)
    row_gate = jnp.where(pick, plan[:, :, None, :], 0.0).sum(axis=3)

    blocks = jnp.stack(ring_gathered(normed, "ep"))
    taken = jnp.einsum("sjct,std->jscd", picker, blocks, preferred_element_type=F32).astype(BF)
    taken = taken.reshape(local, ep * capacity, width)
    half = ep * capacity // 2
    own_rows = lax.dynamic_index_in_dim(taken, mine, 0, keepdims=False)
    other_rows = lax.dynamic_index_in_dim(taken, other, 0, keepdims=False)

    def core_pair(x):
        return lax.ppermute(x, "tp", [(i, i ^ 1) for i in range(tp)])

    def chips_met(own, for_next):
        from_up = sent(for_next, "tp", -2)
        from_down = sent(for_next, "tp", 2)
        far = sent(own, "tp", 4)
        seen = [own, from_up, from_down, far]
        return seen + [core_pair(b) for b in seen]

    chip_order = [chip, (chip + 1) % (tp // 2), (chip - 1) % (tp // 2), (chip + 2) % (tp // 2)]
    order = [2 * c + core for c in chip_order] + [2 * c + 1 - core for c in chip_order]

    def rows_of(w, at, size):
        return jnp.concatenate([lax.dynamic_slice_in_dim(w, i * size, size, 0) for i in at], axis=0)

    gate_up = jnp.concatenate(
        [kept[:, :units], swapped[:, :units], kept[:, units:], swapped[:, units:]], axis=1
    )
    gate_up = rows_of(gate_up, order, width)
    features = jnp.concatenate(chips_met(own_rows, other_rows), axis=1)
    both = jnp.dot(features, gate_up, preferred_element_type=F32)
    gate_val, up_val = both[:, : 2 * units], both[:, 2 * units :]
    hidden = (jax.nn.silu(gate_val) * up_val).astype(BF)

    met = chips_met(hidden, hidden)
    mine_hidden = jnp.concatenate([met[0], met[3], met[4], met[7]], axis=1)
    other_hidden = jnp.concatenate([met[1], met[2], met[5], met[6]], axis=1)

    def slices_at(c, k):
        return [2 * c + k, (2 * (c + 1 - 2 * k) + k) % tp]

    own_order = [i for k in (core, 1 - core) for c in (chip, chip + 2) for i in slices_at(c, k)]
    other_order = [i for k in (core, 1 - core) for c in (chip + 1, chip - 1) for i in slices_at(c, k)]
    own_down = rows_of(lax.dynamic_index_in_dim(down_weight, mine, 0, keepdims=False), [i % tp for i in own_order], units)
    other_down = rows_of(lax.dynamic_index_in_dim(down_weight, other, 0, keepdims=False), [i % tp for i in other_order], units)
    own_out = jnp.dot(mine_hidden, own_down, preferred_element_type=F32)
    other_out = jnp.dot(other_hidden, other_down, preferred_element_type=F32)

    def back(out, which):
        gate = lax.dynamic_index_in_dim(row_gate, which, 1, keepdims=False)
        put = lax.dynamic_index_in_dim(picker, which, 1, keepdims=False)
        scaled = (out.reshape(ep, capacity, width) * gate[:, :, None]).astype(BF)
        return jnp.einsum("sct,scd->std", put, scaled, preferred_element_type=F32)

    partial = (back(own_out, mine) + back(other_out, other)).astype(BF)

    step = ep // 4

    def wanted_by(shift):
        return jnp.stack([partial[(shift + step * a) % ep] for a in range(4)])

    near = wanted_by(0).astype(F32)
    for shift in (1, -1, 2):
        near = near + sent(wanted_by(shift), "ep", shift).astype(F32)
    near_low = near.astype(BF)
    mixture = near[0]
    for a in (1, 2, 3):
        mixture = mixture + sent(near_low[a], "ep", step * a).astype(F32)
    return (residual_wide + mixture).astype(BF)


def solution(mesh):
    return jax.shard_map(
        shards,
        mesh=mesh,
        in_specs=(
            P(("rep", "ep"), "tp"),
            P(("rep", "ep"), "tp"),
            P(("rep", "ep"), None),
            P(("rep", "ep"), None),
            P(("rep", "ep")),
            P("tp", "ep"),
            P("tp"),
            P(("rep", "ep"), None),
            P(("rep", "ep"), None),
            P("ep", None, "tp"),
            P("ep", None, "tp"),
            P("ep", None, "tp"),
        ),
        out_specs=P(("rep", "ep"), "tp"),
        check_vma=False,
    )
```

```python
import jax
import jax.numpy as jnp
from jax import lax
from jax.sharding import PartitionSpec as P

HEAD_DIM = 128
KV_HEADS = 2
EPSILON = 1e-06
BF = jnp.bfloat16
F32 = jnp.float32


def sent(x, axis, shift):
    n = lax.axis_size(axis)
    return lax.ppermute(x, axis, [(i, (i + shift) % n) for i in range(n)])


def attend(queries, key_rows, value_rows, seq_lengths):
    seq_rows = queries.shape[0]
    heads_here = queries.shape[1] // HEAD_DIM
    group_size = heads_here * lax.axis_size("tp") // KV_HEADS
    kv_column = lax.axis_index("tp") * heads_here // group_size * HEAD_DIM
    key_head = lax.dynamic_slice_in_dim(key_rows, kv_column, HEAD_DIM, 1)
    value_head = lax.dynamic_slice_in_dim(value_rows, kv_column, HEAD_DIM, 1)
    query_three = queries.reshape(seq_rows, heads_here, HEAD_DIM)
    scores = jnp.einsum(
        "qhd,kd->hqk", query_three, key_head, preferred_element_type=F32
    ) * HEAD_DIM ** (-0.5)
    positions = jnp.arange(seq_rows, dtype=jnp.int32)
    visible = (positions[None, :] <= positions[:, None]) & (positions[None, :] < seq_lengths[0])
    scores = jnp.where(visible[None, :, :], scores, F32(-1e30))
    row_peak = jnp.max(scores, axis=2, keepdims=True)
    exponent = jnp.exp(scores - row_peak)
    weights = (exponent / jnp.sum(exponent, axis=2, keepdims=True)).astype(BF)
    combined = jnp.einsum("hqk,kd->qhd", weights, value_head, preferred_element_type=F32)
    return combined.astype(BF).reshape(seq_rows, heads_here * HEAD_DIM)


def swapped_between(x, axis, step):
    return lax.ppermute(x, axis, [(i, i ^ step) for i in range(lax.axis_size(axis))])


def pair_columns(out_weight):
    odd = lax.axis_index("ep") % 2
    ahead = sent(out_weight, "ep", -2)
    mate = swapped_between(out_weight, "ep", 1)
    ahead_mate = swapped_between(ahead, "ep", 1)

    def ordered(a, b):
        return jnp.concatenate([jnp.where(odd == 0, a, b), jnp.where(odd == 0, b, a)], axis=1)

    return ordered(out_weight, mate), ordered(ahead, ahead_mate)


def project(tokens, columns):
    ep, tp = lax.axis_size("ep"), lax.axis_size("tp")
    t = lax.axis_index("tp")
    chip, core = t // 2, t % 2
    rows = tokens.shape[0] // 4
    kept, given = [jnp.where(core == k, columns[0], columns[1]) for k in (0, 1)]
    leaving = jnp.dot(tokens, given, preferred_element_type=F32).astype(BF)
    staying = jnp.dot(tokens, kept, preferred_element_type=F32)
    chip_sum = (staying + swapped_between(leaving, "tp", 1).astype(F32)).astype(BF).reshape(4, rows, -1)
    total = lax.dynamic_index_in_dim(chip_sum, chip, 0, keepdims=False).astype(F32)
    for r in (1, 2, 3):
        block = lax.dynamic_index_in_dim(chip_sum, (chip + r) % 4, 0, keepdims=False)
        total = total + sent(block, "tp", 2 * r).astype(F32)
    owner = []
    for e in range(ep):
        for t in range(tp):
            e_to, t_to = (e + ep // 4 * (t // 2)) % ep, (e // 2 + t % 2) % tp
            owner.append((e * tp + t, e_to * tp + t_to))
    return lax.ppermute(total.astype(BF), ("ep", "tp"), owner)


FAR = (0, 4, 12, 8)
OFFSETS = FAR + (1, 5, 13, 9) + (15, 3, 11, 7) + (2, 6, 14, 10)


def gathered(x):
    far = jnp.stack([x, sent(x, "ep", -4), sent(x, "ep", 4), sent(x, "ep", 8)])
    return [
        far,
        sent(far, "ep", -1),
        sent(far, "ep", 1),
        sent(far[0:2], "ep", -2),
        sent(jnp.stack([far[0], far[2]]), "ep", 2),
    ]


def summed(parts):
    own, above, below, near_up, near_down = [
        parts[0:4], parts[4:8], parts[8:12], parts[12:14], parts[14:16]
    ]
    up, down = sent(near_up, "ep", 2), sent(near_down, "ep", -2)
    beside = sent(above, "ep", 1).astype(F32) + sent(below, "ep", -1).astype(F32) + own.astype(F32)
    beside = [beside[k] for k in range(4)]
    beside[0] = beside[0] + up[0].astype(F32) + down[0].astype(F32)
    beside[1] = beside[1] + up[1].astype(F32)
    beside[2] = beside[2] + down[1].astype(F32)
    total = beside[0]
    for k, shift in ((3, 8), (1, 4), (2, -4)):
        total = total + sent(beside[k].astype(BF), "ep", shift).astype(F32)
    return total


def shards(
    residual_in,
    queries,
    key_rows,
    value_rows,
    seq_lengths,
    out_weight,
    norm_gain,
    expert_ids,
    gate_probs,
    gate_weight,
    up_weight,
    down_weight,
):
    rows, width = residual_in.shape
    ep, tp = lax.axis_size("ep"), lax.axis_size("tp")
    e, t = lax.axis_index("ep"), lax.axis_index("tp")
    chip, core = t // 2, t % 2
    local, _, units = gate_weight.shape
    experts = local * ep
    top = expert_ids.shape[1]
    capacity = min(rows, 3 * rows * top // (2 * experts))
    mine = chip % 2
    other = 1 - mine

    columns = pair_columns(out_weight)

    def slices(which):
        return jnp.concatenate(
            [lax.dynamic_index_in_dim(w, which, 0, keepdims=False) for w in (gate_weight, up_weight)], axis=1
        )

    kept = slices(mine)
    swapped = lax.ppermute(
        slices(other), "tp", [(i, (i + (2 if i % 2 else -2)) % tp) for i in range(tp)]
    )

    wanted = expert_ids[:, :, None] == jnp.arange(experts, dtype=jnp.int32)[None, None, :]
    chosen = jnp.where(
        wanted.any(axis=1), jnp.where(wanted, gate_probs[:, :, None], 0.0).sum(axis=1), -1.0
    )
    plan = lax.all_to_all(
        chosen.T.reshape(ep, local, rows), "ep", split_axis=0, concat_axis=0, tiled=True
    )

    attended = attend(queries, key_rows, value_rows, seq_lengths)
    tokens = jnp.concatenate(
        [attended] + [sent(attended, "ep", shift) for shift in (-4, 8, 4)], axis=0
    )
    tokens, plan, swapped = lax.optimization_barrier((tokens, plan, swapped))
    head_total = project(tokens, columns)
    residual = (residual_in.astype(F32) + head_total.astype(F32)).astype(BF)
    residual_wide = residual.astype(F32)

    plan = lax.dynamic_slice_in_dim(jnp.concatenate([plan, plan], axis=0), e, ep, 0)
    plan = jnp.stack([plan[k] for k in OFFSETS])
    hit = plan >= 0
    before = jnp.tril(jnp.ones((rows, rows), BF), -1)
    rank = jnp.einsum("sjt,ut->sju", hit.astype(BF), before, preferred_element_type=F32)
    slot = jnp.arange(capacity, dtype=F32)
    pick = (rank[:, :, None, :] == slot[None, None, :, None]) & hit[:, :, None, :]
    picker = pick.astype(BF)
    row_gate = jnp.where(pick, plan[:, :, None, :], 0.0).sum(axis=3)

    blocks = jnp.concatenate(gathered(residual))
    taken = jnp.einsum("sjct,std->jscd", picker, blocks, preferred_element_type=F32)
    taken = taken.reshape(local, ep * capacity, width)
    square_sum = jnp.sum(taken * taken, axis=2)
    high = lax.reduce_precision(square_sum, exponent_bits=8, mantissa_bits=7)
    carried = jnp.stack([high, square_sum - high], axis=1).astype(BF).reshape(local, -1, width)
    extra = carried.shape[1]
    carried = jnp.pad(carried, ((0, 0), (0, -extra % 8), (0, 0)))
    taken = jnp.concatenate([(taken * norm_gain).astype(BF), carried], axis=1)
    own_rows = lax.dynamic_index_in_dim(taken, mine, 0, keepdims=False)
    other_rows = lax.dynamic_index_in_dim(taken, other, 0, keepdims=False)

    def chips_met(own, for_next):
        from_up = sent(for_next, "tp", -2)
        from_down = sent(for_next, "tp", 2)
        far = sent(own, "tp", 4)
        seen = [own, from_up, from_down, far]
        return seen + [swapped_between(b, "tp", 1) for b in seen]

    chip_order = [chip, (chip + 1) % (tp // 2), (chip - 1) % (tp // 2), (chip + 2) % (tp // 2)]
    order = [2 * c + core for c in chip_order] + [2 * c + 1 - core for c in chip_order]

    def rows_of(w, at, size):
        return jnp.concatenate([lax.dynamic_slice_in_dim(w, i * size, size, 0) for i in at], axis=0)

    gate_up = jnp.concatenate(
        [kept[:, :units], swapped[:, :units], kept[:, units:], swapped[:, units:]], axis=1
    )
    gate_up = rows_of(gate_up, order, width)
    count = ep * capacity
    arrived = chips_met(own_rows, other_rows)
    features = jnp.concatenate([b[:count] for b in arrived], axis=1)
    squares = sum(b[count : count + extra].astype(F32).reshape(2, count).sum(axis=0) for b in arrived)
    scale = lax.rsqrt(squares / (width * tp) + EPSILON)
    both = jnp.dot(features, gate_up, preferred_element_type=F32) * scale[:, None]
    gate_val, up_val = both[:, : 2 * units], both[:, 2 * units :]
    hidden = (jax.nn.silu(gate_val) * up_val).astype(BF)

    met = chips_met(hidden, hidden)
    mine_hidden = jnp.concatenate([met[0], met[3], met[4], met[7]], axis=1)
    other_hidden = jnp.concatenate([met[1], met[2], met[5], met[6]], axis=1)

    def slices_at(c, k):
        return [2 * c + k, (2 * (c + 1 - 2 * k) + k) % tp]

    own_order = [i for k in (core, 1 - core) for c in (chip, chip + 2) for i in slices_at(c, k)]
    other_order = [i for k in (core, 1 - core) for c in (chip + 1, chip - 1) for i in slices_at(c, k)]
    own_down = rows_of(lax.dynamic_index_in_dim(down_weight, mine, 0, keepdims=False), [i % tp for i in own_order], units)
    other_down = rows_of(lax.dynamic_index_in_dim(down_weight, other, 0, keepdims=False), [i % tp for i in other_order], units)
    own_out = jnp.dot(mine_hidden, own_down, preferred_element_type=F32)
    other_out = jnp.dot(other_hidden, other_down, preferred_element_type=F32)

    def back(out, which):
        gate = lax.dynamic_index_in_dim(row_gate, which, 1, keepdims=False)
        put = lax.dynamic_index_in_dim(picker, which, 1, keepdims=False)
        scaled = (out.reshape(ep, capacity, width) * gate[:, :, None]).astype(BF)
        return jnp.einsum("sct,scd->std", put, scaled, preferred_element_type=F32)

    partial = (back(own_out, mine) + back(other_out, other)).astype(BF)
    return (residual_wide + summed(partial)).astype(BF)


def solution(mesh):
    return jax.shard_map(
        shards,
        mesh=mesh,
        in_specs=(
            P(("rep", "ep"), "tp"),
            P(("rep", "ep"), "tp"),
            P(("rep", "ep"), None),
            P(("rep", "ep"), None),
            P(("rep", "ep")),
            P("tp", "ep"),
            P("tp"),
            P(("rep", "ep"), None),
            P(("rep", "ep"), None),
            P("ep", None, "tp"),
            P("ep", None, "tp"),
            P("ep", None, "tp"),
        ),
        out_specs=P(("rep", "ep"), "tp"),
        check_vma=False,
    )
```

```python
import jax
import jax.numpy as jnp
from jax import lax
from jax.sharding import PartitionSpec as P


HEAD_DIM = 128
KV_HEADS = 2
EPSILON = 1e-06
BF = jnp.bfloat16
F32 = jnp.float32


def sent(x, axis, shift):
    n = lax.axis_size(axis)
    return lax.ppermute(x, axis, [(i, (i + shift) % n) for i in range(n)])


def attend(queries, key_rows, value_rows, seq_lengths):
    seq_rows = queries.shape[0]
    heads_here = queries.shape[1] // HEAD_DIM
    group_size = heads_here * lax.axis_size("tp") // KV_HEADS
    kv_column = lax.axis_index("tp") * heads_here // group_size * HEAD_DIM
    key_head = lax.dynamic_slice_in_dim(key_rows, kv_column, HEAD_DIM, 1)
    value_head = lax.dynamic_slice_in_dim(value_rows, kv_column, HEAD_DIM, 1)
    query_three = queries.reshape(seq_rows, heads_here, HEAD_DIM)
    scores = jnp.einsum(
        "qhd,kd->hqk", query_three, key_head, preferred_element_type=F32
    ) * HEAD_DIM ** (-0.5)
    positions = jnp.arange(seq_rows, dtype=jnp.int32)
    visible = (positions[None, :] <= positions[:, None]) & (positions[None, :] < seq_lengths[0])
    scores = jnp.where(visible[None, :, :], scores, F32(-1e30))
    row_peak = jnp.max(scores, axis=2, keepdims=True)
    exponent = jnp.exp(scores - row_peak)
    weights = (exponent / jnp.sum(exponent, axis=2, keepdims=True)).astype(BF)
    combined = jnp.einsum("hqk,kd->qhd", weights, value_head, preferred_element_type=F32)
    return combined.astype(BF).reshape(seq_rows, heads_here * HEAD_DIM)


def swapped_between(x, axis, step):
    return lax.ppermute(x, axis, [(i, i ^ step) for i in range(lax.axis_size(axis))])


def pair_columns(out_weight):
    odd = lax.axis_index("ep") % 2
    ahead = sent(out_weight, "ep", -2)
    mate = swapped_between(out_weight, "ep", 1)
    ahead_mate = swapped_between(ahead, "ep", 1)

    def ordered(a, b):
        return jnp.concatenate([jnp.where(odd == 0, a, b), jnp.where(odd == 0, b, a)], axis=1)

    return ordered(out_weight, mate), ordered(ahead, ahead_mate)


def project(tokens, columns):
    ep, tp = lax.axis_size("ep"), lax.axis_size("tp")
    t = lax.axis_index("tp")
    chip, core = t // 2, t % 2
    rows = tokens.shape[0] // 4
    kept, given = [jnp.where(core == k, columns[0], columns[1]) for k in (0, 1)]
    leaving = jnp.dot(tokens, given, preferred_element_type=F32).astype(BF)
    staying = jnp.dot(tokens, kept, preferred_element_type=F32)
    chip_sum = (staying + swapped_between(leaving, "tp", 1).astype(F32)).astype(BF).reshape(4, rows, -1)
    total = lax.dynamic_index_in_dim(chip_sum, chip, 0, keepdims=False).astype(F32)
    for r in (1, 2, 3):
        block = lax.dynamic_index_in_dim(chip_sum, (chip + r) % 4, 0, keepdims=False)
        total = total + sent(block, "tp", 2 * r).astype(F32)
    owner = []
    for e in range(ep):
        for t in range(tp):
            e_to, t_to = (e + ep // 4 * (t // 2)) % ep, (e // 2 + t % 2) % tp
            owner.append((e * tp + t, e_to * tp + t_to))
    return lax.ppermute(total.astype(BF), ("ep", "tp"), owner)


def quarter_ring(n):
    return [[k * 4 + c for k in range(n // 4)] for c in range(4)]


def gathered(x):
    far = lax.all_to_all(
        jnp.broadcast_to(x[None], (4, *x.shape)), "ep", 0, 0,
        axis_index_groups=quarter_ring(lax.axis_size("ep")), tiled=True,
    )
    return [
        far,
        sent(far, "ep", -1),
        sent(far, "ep", 1),
        sent(far[:2], "ep", -2),
        sent(far[2:], "ep", 2),
    ]


def summed(own, above, below, opposite):
    up, down = sent(opposite[:2], "ep", 2), sent(opposite[2:], "ep", -2)
    beside = own.astype(F32) + sent(above, "ep", 1).astype(F32) + sent(below, "ep", -1).astype(F32)
    beside = beside + jnp.concatenate([up, down]).astype(F32)
    place = lax.axis_index("ep") // 4
    total = lax.dynamic_index_in_dim(beside, place, 0, keepdims=False)
    for step in (2, 1, 3):
        block = lax.dynamic_index_in_dim(beside, (place + step) % 4, 0, keepdims=False)
        total = total + sent(block.astype(BF), "ep", 4 * step).astype(F32)
    return total


def shards(
    residual_in,
    queries,
    key_rows,
    value_rows,
    seq_lengths,
    out_weight,
    norm_gain,
    expert_ids,
    gate_probs,
    gate_weight,
    up_weight,
    down_weight,
):
    rows, width = residual_in.shape
    ep, tp = lax.axis_size("ep"), lax.axis_size("tp")
    e, t = lax.axis_index("ep"), lax.axis_index("tp")
    chip, core = t // 2, t % 2
    local, _, units = gate_weight.shape
    experts = local * ep
    top = expert_ids.shape[1]
    capacity = min(rows, 3 * rows * top // (2 * experts))
    mine = chip % 2
    other = 1 - mine

    columns = pair_columns(out_weight)

    def slices(which):
        return jnp.concatenate(
            [lax.dynamic_index_in_dim(w, which, 0, keepdims=False) for w in (gate_weight, up_weight)], axis=1
        )

    kept = slices(mine)
    swapped = lax.ppermute(
        slices(other), "tp", [(i, (i + (2 if i % 2 else -2)) % tp) for i in range(tp)]
    )
    chip_order = [chip, (chip + 1) % (tp // 2), (chip - 1) % (tp // 2), (chip + 2) % (tp // 2)]
    order = [2 * c + core for c in chip_order] + [2 * c + 1 - core for c in chip_order]
    gate_up = jnp.concatenate(
        [kept[:, :units], swapped[:, :units], kept[:, units:], swapped[:, units:]], axis=1
    )
    gate_up = [lax.dynamic_slice_in_dim(gate_up, i * width, width, 0) for i in order]

    wanted = expert_ids[:, :, None] == jnp.arange(experts, dtype=jnp.int32)[None, None, :]
    chosen = jnp.where(
        wanted.any(axis=1), jnp.where(wanted, gate_probs[:, :, None], 0.0).sum(axis=1), -1.0
    )
    plan = lax.all_to_all(
        chosen.T.reshape(ep, local, rows), "ep", split_axis=0, concat_axis=0, tiled=True
    )

    attended = attend(queries, key_rows, value_rows, seq_lengths)
    tokens = [attended] + [sent(attended, "ep", shift) for shift in (-4, 8, 4)]
    tokens, plan, gate_up = lax.optimization_barrier((tokens, plan, gate_up))
    tokens = jnp.concatenate(tokens, axis=0)
    head_total = project(tokens, columns)
    residual = (residual_in.astype(F32) + head_total.astype(F32)).astype(BF)
    residual_wide = residual.astype(F32)

    classes = [(e + k) % 4 for k in (0, 1, 3, 2)]
    plan = plan.reshape(ep // 4, 4, local, rows)
    plan = jnp.concatenate([lax.dynamic_index_in_dim(plan, c, 1, keepdims=False) for c in classes])
    slot = jnp.arange(capacity, dtype=F32)
    before = jnp.tril(jnp.ones((rows, rows), BF), -1)

    def rows_for(which):
        gate = lax.dynamic_index_in_dim(plan, which, 1, keepdims=False)
        hit = gate >= 0
        rank = jnp.einsum("st,ut->su", hit.astype(BF), before, preferred_element_type=F32)
        pick = (rank[:, None, :] == slot[None, :, None]) & hit[:, None, :]
        return pick, jnp.where(pick, gate[:, None, :], 0.0).sum(axis=2)

    picks, row_gates = zip(rows_for(mine), rows_for(other))
    picks, row_gates = lax.optimization_barrier((picks, row_gates))
    blocks = jnp.concatenate(gathered(residual))
    block_squares = jnp.sum(jnp.square(blocks.astype(F32)), axis=2)

    def message(pick):
        taken = jnp.einsum("sct,std->scd", pick.astype(BF), blocks, preferred_element_type=F32)
        taken = (taken.reshape(-1, width) * norm_gain).astype(BF)
        square_sum = jnp.where(pick, block_squares[:, None, :], 0.0).sum(axis=2).reshape(-1)
        high = lax.reduce_precision(square_sum, exponent_bits=8, mantissa_bits=7)
        carried = jnp.stack([high, square_sum - high]).astype(BF).reshape(-1, width)
        return jnp.concatenate([taken, jnp.pad(carried, ((0, -carried.shape[0] % 8), (0, 0)))])

    own_rows, other_rows = message(picks[0]), message(picks[1])

    def chips_met(own, for_next):
        from_up = sent(for_next, "tp", -2)
        from_down = sent(for_next, "tp", 2)
        far = sent(own, "tp", 4)
        seen = [own, from_up, from_down, far]
        return seen + [swapped_between(b, "tp", 1) for b in seen]

    def rows_of(w, at, size):
        return jnp.concatenate([lax.dynamic_slice_in_dim(w, i * size, size, 0) for i in at], axis=0)

    count = ep * capacity
    extra = 2 * count // width
    arrived = chips_met(own_rows, other_rows)
    both = jnp.zeros((count, 4 * units), F32)
    for k in (0, 4, 1, 2, 5, 6, 3, 7):
        both = both + jnp.dot(arrived[k][:count], gate_up[k], preferred_element_type=F32)
    squares = sum(b[count : count + extra].astype(F32).reshape(2, count).sum(axis=0) for b in arrived)
    both = both * lax.rsqrt(squares / (width * tp) + EPSILON)[:, None]
    gate_val, up_val = both[:, : 2 * units], both[:, 2 * units :]
    hidden = (jax.nn.silu(gate_val) * up_val).astype(BF)

    met = chips_met(hidden, hidden)
    mine_hidden = jnp.concatenate([met[0], met[3], met[4], met[7]], axis=1)
    other_hidden = jnp.concatenate([met[1], met[2], met[5], met[6]], axis=1)

    def slices_at(c, k):
        return [2 * c + k, (2 * (c + 1 - 2 * k) + k) % tp]

    own_order = [i for k in (core, 1 - core) for c in (chip, chip + 2) for i in slices_at(c, k)]
    other_order = [i for k in (core, 1 - core) for c in (chip + 1, chip - 1) for i in slices_at(c, k)]
    own_down = rows_of(lax.dynamic_index_in_dim(down_weight, mine, 0, keepdims=False), [i % tp for i in own_order], units)
    other_down = rows_of(lax.dynamic_index_in_dim(down_weight, other, 0, keepdims=False), [i % tp for i in other_order], units)
    own_out = jnp.dot(mine_hidden, own_down, preferred_element_type=F32)
    other_out = jnp.dot(other_hidden, other_down, preferred_element_type=F32)

    def back(k, out):
        scaled = (out.reshape(ep, capacity, width) * row_gates[k][:, :, None]).astype(BF)
        return jnp.einsum("sct,scd->std", picks[k].astype(BF), scaled, preferred_element_type=F32)

    partial = (back(0, own_out) + back(1, other_out)).astype(BF)
    return (residual_wide + summed(*jnp.split(partial, 4))).astype(BF)


def solution(mesh):
    return jax.shard_map(
        shards,
        mesh=mesh,
        in_specs=(
            P(("rep", "ep"), "tp"),
            P(("rep", "ep"), "tp"),
            P(("rep", "ep"), None),
            P(("rep", "ep"), None),
            P(("rep", "ep")),
            P("tp", "ep"),
            P("tp"),
            P(("rep", "ep"), None),
            P(("rep", "ep"), None),
            P("ep", None, "tp"),
            P("ep", None, "tp"),
            P("ep", None, "tp"),
        ),
        out_specs=P(("rep", "ep"), "tp"),
        check_vma=False,
    )
```

```python
import jax
import jax.numpy as jnp
from jax import lax
from jax.sharding import PartitionSpec as P


HEAD_DIM = 128
KV_HEADS = 2
EPSILON = 1e-06
BF = jnp.bfloat16
F32 = jnp.float32


def sent(x, axis, shift):
    n = lax.axis_size(axis)
    return lax.ppermute(x, axis, [(i, (i + shift) % n) for i in range(n)])


def attend(queries, key_rows, value_rows, seq_lengths):
    seq_rows = queries.shape[0]
    heads_here = queries.shape[1] // HEAD_DIM
    group_size = heads_here * lax.axis_size("tp") // KV_HEADS
    kv_column = lax.axis_index("tp") * heads_here // group_size * HEAD_DIM
    key_head = lax.dynamic_slice_in_dim(key_rows, kv_column, HEAD_DIM, 1)
    value_head = lax.dynamic_slice_in_dim(value_rows, kv_column, HEAD_DIM, 1)
    query_three = queries.reshape(seq_rows, heads_here, HEAD_DIM)
    scores = jnp.einsum(
        "qhd,kd->hqk", query_three, key_head, preferred_element_type=F32
    ) * HEAD_DIM ** (-0.5)
    positions = jnp.arange(seq_rows, dtype=jnp.int32)
    visible = (positions[None, :] <= positions[:, None]) & (positions[None, :] < seq_lengths[0])
    scores = jnp.where(visible[None, :, :], scores, F32(-1e30))
    row_peak = jnp.max(scores, axis=2, keepdims=True)
    exponent = jnp.exp(scores - row_peak)
    weights = (exponent / jnp.sum(exponent, axis=2, keepdims=True)).astype(BF)
    combined = jnp.einsum("hqk,kd->qhd", weights, value_head, preferred_element_type=F32)
    return combined.astype(BF).reshape(seq_rows, heads_here * HEAD_DIM)


def swapped_between(x, axis, step):
    return lax.ppermute(x, axis, [(i, i ^ step) for i in range(lax.axis_size(axis))])


def pair_columns(out_weight):
    odd = lax.axis_index("ep") % 2
    ahead = sent(out_weight, "ep", -2)
    mate = swapped_between(out_weight, "ep", 1)
    ahead_mate = swapped_between(ahead, "ep", 1)

    def ordered(a, b):
        return jnp.concatenate([jnp.where(odd == 0, a, b), jnp.where(odd == 0, b, a)], axis=1)

    return ordered(out_weight, mate), ordered(ahead, ahead_mate)


def project(tokens, columns):
    t = lax.axis_index("tp")
    chip, core = t // 2, t % 2
    rows = tokens.shape[0] // 4
    kept, given = [jnp.where(core == k, columns[0], columns[1]) for k in (0, 1)]
    leaving = jnp.dot(tokens, given, preferred_element_type=F32).astype(BF)
    staying = jnp.dot(tokens, kept, preferred_element_type=F32)
    chip_sum = (staying + swapped_between(leaving, "tp", 1).astype(F32)).astype(BF).reshape(4, rows, -1)
    total = lax.dynamic_index_in_dim(chip_sum, chip, 0, keepdims=False).astype(F32)
    for r in (1, 2, 3):
        block = lax.dynamic_index_in_dim(chip_sum, (chip + r) % 4, 0, keepdims=False)
        total = total + sent(block, "tp", 2 * r).astype(F32)
    return total


FAR = (0, 4, 12, 8)
OFFSETS = FAR + (1, 5, 13, 9) + (15, 3, 11, 7) + (2, 6, 14, 10)


def holder_moves(shift):
    ep, tp = lax.axis_size("ep"), lax.axis_size("tp")
    return [
        (e * tp + t, (e + ep // 4 * (t // 2) + shift) % ep * tp + (e // 2 + t % 2) % tp)
        for e in range(ep)
        for t in range(tp)
    ]


def gathered(held):
    far = [lax.ppermute(held, ("ep", "tp"), holder_moves(-shift)) for shift in FAR]
    level = jnp.stack(far)
    return far[0], [
        level,
        sent(level, "ep", -1),
        sent(level, "ep", 1),
        sent(level[0:2], "ep", -2),
        sent(jnp.stack([far[0], far[2]]), "ep", 2),
    ]


def summed(parts):
    own, above, below, near_up, near_down = [
        parts[0:4], parts[4:8], parts[8:12], parts[12:14], parts[14:16]
    ]
    up, down = sent(near_up, "ep", 2), sent(near_down, "ep", -2)
    beside = sent(above, "ep", 1).astype(F32) + sent(below, "ep", -1).astype(F32) + own.astype(F32)
    beside = [beside[k] for k in range(4)]
    beside[0] = beside[0] + up[0].astype(F32) + down[0].astype(F32)
    beside[1] = beside[1] + up[1].astype(F32)
    beside[2] = beside[2] + down[1].astype(F32)
    total = beside[0]
    for k, shift in ((3, 8), (1, 4), (2, -4)):
        total = total + sent(beside[k].astype(BF), "ep", shift).astype(F32)
    return total


def shards(
    residual_in,
    queries,
    key_rows,
    value_rows,
    seq_lengths,
    out_weight,
    norm_gain,
    expert_ids,
    gate_probs,
    gate_weight,
    up_weight,
    down_weight,
):
    rows, width = residual_in.shape
    ep, tp = lax.axis_size("ep"), lax.axis_size("tp")
    e, t = lax.axis_index("ep"), lax.axis_index("tp")
    chip, core = t // 2, t % 2
    local, _, units = gate_weight.shape
    experts = local * ep
    top = expert_ids.shape[1]
    capacity = min(rows, 3 * rows * top // (2 * experts))
    mine = chip % 2
    other = 1 - mine

    columns = pair_columns(out_weight)

    def slices(which):
        return jnp.concatenate(
            [lax.dynamic_index_in_dim(w, which, 0, keepdims=False) for w in (gate_weight, up_weight)], axis=1
        )

    kept = slices(mine)
    swapped = lax.ppermute(
        slices(other), "tp", [(i, (i + (2 if i % 2 else -2)) % tp) for i in range(tp)]
    )
    chip_order = [chip, (chip + 1) % (tp // 2), (chip - 1) % (tp // 2), (chip + 2) % (tp // 2)]
    order = [2 * c + core for c in chip_order] + [2 * c + 1 - core for c in chip_order]
    gate_up = jnp.concatenate(
        [kept[:, :units], swapped[:, :units], kept[:, units:], swapped[:, units:]], axis=1
    )
    gate_up = jnp.concatenate([lax.dynamic_slice_in_dim(gate_up, i * width, width, 0) for i in order], axis=0)

    wanted = expert_ids[:, :, None] == jnp.arange(experts, dtype=jnp.int32)[None, None, :]
    chosen = jnp.where(
        wanted.any(axis=1), jnp.where(wanted, gate_probs[:, :, None], 0.0).sum(axis=1), -1.0
    )
    plan = lax.all_to_all(
        chosen.T.reshape(ep, local, rows), "ep", split_axis=0, concat_axis=0, tiled=True
    )

    attended = attend(queries, key_rows, value_rows, seq_lengths)
    tokens = [attended] + [sent(attended, "ep", shift) for shift in (-4, 8, 4)]
    residual_held = lax.ppermute(
        residual_in, ("ep", "tp"), [(to, at) for at, to in holder_moves(0)]
    )
    tokens, plan = lax.optimization_barrier((tokens, plan))
    tokens = jnp.concatenate(tokens, axis=0)
    held = (residual_held.astype(F32) + project(tokens, columns)).astype(BF)

    plan = lax.dynamic_slice_in_dim(jnp.concatenate([plan, plan], axis=0), e, ep, 0)
    plan = jnp.stack([plan[k] for k in OFFSETS])
    slot = jnp.arange(capacity, dtype=F32)
    before = jnp.tril(jnp.ones((rows, rows), BF), -1)

    def rows_for(which):
        gate = lax.dynamic_index_in_dim(plan, which, 1, keepdims=False)
        hit = gate >= 0
        rank = jnp.einsum("st,ut->su", hit.astype(BF), before, preferred_element_type=F32)
        pick = (rank[:, None, :] == slot[None, :, None]) & hit[:, None, :]
        return pick, jnp.where(pick, gate[:, None, :], 0.0).sum(axis=2)

    picks, row_gates = zip(rows_for(mine), rows_for(other))
    picks, row_gates = lax.optimization_barrier((picks, row_gates))
    residual, blocks = gathered(held)
    blocks, gate_up = lax.optimization_barrier((blocks, gate_up))
    blocks = jnp.concatenate(blocks)
    block_squares = jnp.sum(jnp.square(blocks.astype(F32)), axis=2)

    def message(pick):
        taken = jnp.einsum("sct,std->scd", pick.astype(BF), blocks, preferred_element_type=F32)
        taken = (taken.reshape(-1, width) * norm_gain).astype(BF)
        square_sum = jnp.where(pick, block_squares[:, None, :], 0.0).sum(axis=2).reshape(-1)
        high = lax.reduce_precision(square_sum, exponent_bits=8, mantissa_bits=7)
        carried = jnp.stack([high, square_sum - high]).astype(BF).reshape(-1, width)
        return jnp.concatenate([taken, jnp.pad(carried, ((0, -carried.shape[0] % 8), (0, 0)))])

    own_rows, other_rows = message(picks[0]), message(picks[1])

    def chips_met(own, for_next):
        from_up = sent(for_next, "tp", -2)
        from_down = sent(for_next, "tp", 2)
        far = sent(own, "tp", 4)
        seen = [own, from_up, from_down, far]
        return seen + [swapped_between(b, "tp", 1) for b in seen]

    def rows_of(w, at, size):
        return jnp.concatenate([lax.dynamic_slice_in_dim(w, i * size, size, 0) for i in at], axis=0)

    count = ep * capacity
    extra = 2 * count // width
    features = jnp.concatenate(chips_met(own_rows, other_rows), axis=1)
    both = jnp.dot(features, gate_up, preferred_element_type=F32)[:count]
    squares = features[count : count + extra].astype(F32).reshape(extra, tp, width).sum(axis=1)
    squares = squares.reshape(2, count).sum(axis=0)
    both = both * lax.rsqrt(squares / (width * tp) + EPSILON)[:, None]
    gate_val, up_val = both[:, : 2 * units], both[:, 2 * units :]
    hidden = (jax.nn.silu(gate_val) * up_val).astype(BF)

    met = chips_met(hidden, hidden)
    mine_hidden = jnp.concatenate([met[0], met[3], met[4], met[7]], axis=1)
    other_hidden = jnp.concatenate([met[1], met[2], met[5], met[6]], axis=1)

    def slices_at(c, k):
        return [2 * c + k, (2 * (c + 1 - 2 * k) + k) % tp]

    own_order = [i for k in (core, 1 - core) for c in (chip, chip + 2) for i in slices_at(c, k)]
    other_order = [i for k in (core, 1 - core) for c in (chip + 1, chip - 1) for i in slices_at(c, k)]
    own_down = rows_of(lax.dynamic_index_in_dim(down_weight, mine, 0, keepdims=False), [i % tp for i in own_order], units)
    other_down = rows_of(lax.dynamic_index_in_dim(down_weight, other, 0, keepdims=False), [i % tp for i in other_order], units)
    own_out = jnp.dot(mine_hidden, own_down, preferred_element_type=F32)
    other_out = jnp.dot(other_hidden, other_down, preferred_element_type=F32)

    def back(k, out):
        scaled = (out.reshape(ep, capacity, width) * row_gates[k][:, :, None]).astype(BF)
        return jnp.einsum("sct,scd->std", picks[k].astype(BF), scaled, preferred_element_type=F32)

    partial = (back(0, own_out) + back(1, other_out)).astype(BF)
    return (residual.astype(F32) + summed(partial)).astype(BF)


def solution(mesh):
    return jax.shard_map(
        shards,
        mesh=mesh,
        in_specs=(
            P(("rep", "ep"), "tp"),
            P(("rep", "ep"), "tp"),
            P(("rep", "ep"), None),
            P(("rep", "ep"), None),
            P(("rep", "ep")),
            P("tp", "ep"),
            P("tp"),
            P(("rep", "ep"), None),
            P(("rep", "ep"), None),
            P("ep", None, "tp"),
            P("ep", None, "tp"),
            P("ep", None, "tp"),
        ),
        out_specs=P(("rep", "ep"), "tp"),
        check_vma=False,
    )
```

```python
import jax
import jax.numpy as jnp
from jax import lax
from jax.sharding import PartitionSpec as P


HEAD_DIM = 128
KV_HEADS = 2
EPSILON = 1e-06
BF = jnp.bfloat16
F32 = jnp.float32


def sent(x, axis, shift):
    n = lax.axis_size(axis)
    return lax.ppermute(x, axis, [(i, (i + shift) % n) for i in range(n)])


def attend(queries, key_rows, value_rows, seq_lengths):
    seq_rows = queries.shape[0]
    heads_here = queries.shape[1] // HEAD_DIM
    group_size = heads_here * lax.axis_size("tp") // KV_HEADS
    kv_column = lax.axis_index("tp") * heads_here // group_size * HEAD_DIM
    key_head = lax.dynamic_slice_in_dim(key_rows, kv_column, HEAD_DIM, 1)
    value_head = lax.dynamic_slice_in_dim(value_rows, kv_column, HEAD_DIM, 1)
    query_three = queries.reshape(seq_rows, heads_here, HEAD_DIM)
    scores = jnp.einsum(
        "qhd,kd->hqk", query_three, key_head, preferred_element_type=F32
    ) * HEAD_DIM ** (-0.5)
    positions = jnp.arange(seq_rows, dtype=jnp.int32)
    visible = (positions[None, :] <= positions[:, None]) & (positions[None, :] < seq_lengths[0])
    scores = jnp.where(visible[None, :, :], scores, F32(-1e30))
    row_peak = jnp.max(scores, axis=2, keepdims=True)
    exponent = jnp.exp(scores - row_peak)
    weights = (exponent / jnp.sum(exponent, axis=2, keepdims=True)).astype(BF)
    combined = jnp.einsum("hqk,kd->qhd", weights, value_head, preferred_element_type=F32)
    return combined.astype(BF).reshape(seq_rows, heads_here * HEAD_DIM)


def swapped_between(x, axis, step):
    return lax.ppermute(x, axis, [(i, i ^ step) for i in range(lax.axis_size(axis))])


def pair_columns(out_weight):
    odd = lax.axis_index("ep") % 2
    ahead = sent(out_weight, "ep", -2)
    mate = swapped_between(out_weight, "ep", 1)
    ahead_mate = swapped_between(ahead, "ep", 1)

    def ordered(a, b):
        return jnp.concatenate([jnp.where(odd == 0, a, b), jnp.where(odd == 0, b, a)], axis=1)

    return ordered(out_weight, mate), ordered(ahead, ahead_mate)


def project(tokens, columns):
    t = lax.axis_index("tp")
    chip, core = t // 2, t % 2
    rows = tokens.shape[0] // 4
    kept, given = [jnp.where(core == k, columns[0], columns[1]) for k in (0, 1)]
    leaving = jnp.dot(tokens, given, preferred_element_type=F32).astype(BF)
    staying = jnp.dot(tokens, kept, preferred_element_type=F32)
    chip_sum = (staying + swapped_between(leaving, "tp", 1).astype(F32)).astype(BF).reshape(4, rows, -1)
    total = lax.dynamic_index_in_dim(chip_sum, chip, 0, keepdims=False).astype(F32)
    for r in (1, 2, 3):
        block = lax.dynamic_index_in_dim(chip_sum, (chip + r) % 4, 0, keepdims=False)
        total = total + sent(block, "tp", 2 * r).astype(F32)
    return total


FAR = (0, 4, 12, 8)
OFFSETS = FAR + (1, 5, 13, 9) + (15, 3, 11, 7) + (2, 6, 14, 10)


def holder_moves(shift):
    ep, tp = lax.axis_size("ep"), lax.axis_size("tp")
    return [
        (e * tp + t, (e + ep // 4 * (t // 2) + shift) % ep * tp + (e // 2 + t % 2) % tp)
        for e in range(ep)
        for t in range(tp)
    ]


def gathered(held):
    far = [lax.ppermute(held, ("ep", "tp"), holder_moves(-shift)) for shift in FAR]
    level = jnp.stack(far)
    return far[0], [
        level,
        sent(level, "ep", -1),
        sent(level, "ep", 1),
        sent(level[0:2], "ep", -2),
        sent(jnp.stack([far[0], far[2]]), "ep", 2),
    ]


def summed(parts):
    own, above, below, near_up, near_down = [
        parts[0:4], parts[4:8], parts[8:12], parts[12:14], parts[14:16]
    ]
    up, down = sent(near_up, "ep", 2), sent(near_down, "ep", -2)
    beside = sent(above, "ep", 1).astype(F32) + sent(below, "ep", -1).astype(F32) + own.astype(F32)
    beside = [beside[k] for k in range(4)]
    beside[0] = beside[0] + up[0].astype(F32) + down[0].astype(F32)
    beside[1] = beside[1] + up[1].astype(F32)
    beside[2] = beside[2] + down[1].astype(F32)
    total = beside[0]
    for k, shift in ((3, 8), (1, 4), (2, -4)):
        total = total + sent(beside[k].astype(BF), "ep", shift).astype(F32)
    return total


def shards(
    residual_in,
    queries,
    key_rows,
    value_rows,
    seq_lengths,
    out_weight,
    norm_gain,
    expert_ids,
    gate_probs,
    gate_weight,
    up_weight,
    down_weight,
):
    rows, width = residual_in.shape
    ep, tp = lax.axis_size("ep"), lax.axis_size("tp")
    e, t = lax.axis_index("ep"), lax.axis_index("tp")
    chip, core = t // 2, t % 2
    local, _, units = gate_weight.shape
    experts = local * ep
    top = expert_ids.shape[1]
    capacity = min(rows, 3 * rows * top // (2 * experts))
    mine = chip % 2
    other = 1 - mine

    columns = pair_columns(out_weight)

    wanted = expert_ids[:, :, None] == jnp.arange(experts, dtype=jnp.int32)[None, None, :]
    chosen = jnp.where(
        wanted.any(axis=1), jnp.where(wanted, gate_probs[:, :, None], 0.0).sum(axis=1), -1.0
    )
    plan = lax.all_to_all(
        chosen.T.reshape(ep, local, rows), "ep", split_axis=0, concat_axis=0, tiled=True
    )

    attended = attend(queries, key_rows, value_rows, seq_lengths)
    tokens = [attended] + [sent(attended, "ep", shift) for shift in (-4, 8, 4)]
    residual_held = lax.ppermute(
        residual_in, ("ep", "tp"), [(to, at) for at, to in holder_moves(0)]
    )
    tokens = jnp.concatenate(tokens, axis=0)
    columns, plan = lax.optimization_barrier((columns, plan))
    held = (residual_held.astype(F32) + project(tokens, columns)).astype(BF)
    held, plan, gate_weight, up_weight = lax.optimization_barrier((held, plan, gate_weight, up_weight))

    def slices(which):
        return jnp.concatenate(
            [lax.dynamic_index_in_dim(w, which, 0, keepdims=False) for w in (gate_weight, up_weight)], axis=1
        )

    kept = slices(mine)
    swapped = lax.ppermute(
        slices(other), "tp", [(i, (i + (2 if i % 2 else -2)) % tp) for i in range(tp)]
    )
    chip_order = [chip, (chip + 1) % (tp // 2), (chip - 1) % (tp // 2), (chip + 2) % (tp // 2)]
    order = [2 * c + k for c in chip_order for k in (core, 1 - core)]
    gate_up = jnp.concatenate(
        [kept[:, :units], swapped[:, :units], kept[:, units:], swapped[:, units:]], axis=1
    )
    gate_up = [lax.dynamic_slice_in_dim(gate_up, i * width, width, 0) for i in order]
    gate_up = [jnp.concatenate(gate_up[:6]), jnp.concatenate(gate_up[6:])]

    plan = lax.dynamic_slice_in_dim(jnp.concatenate([plan, plan], axis=0), e, ep, 0)
    plan = jnp.stack([plan[k] for k in OFFSETS])
    slot = jnp.arange(capacity, dtype=F32)
    before = jnp.tril(jnp.ones((rows, rows), BF), -1)

    def rows_for(which):
        gate = lax.dynamic_index_in_dim(plan, which, 1, keepdims=False)
        hit = gate >= 0
        rank = jnp.einsum("st,ut->su", hit.astype(BF), before, preferred_element_type=F32)
        pick = (rank[:, None, :] == slot[None, :, None]) & hit[:, None, :]
        return pick, jnp.where(pick, gate[:, None, :], 0.0).sum(axis=2)

    picks, row_gates = zip(rows_for(mine), rows_for(other))
    picks, row_gates = lax.optimization_barrier((picks, row_gates))
    residual, blocks = gathered(held)
    blocks, gate_up = lax.optimization_barrier((blocks, gate_up))
    blocks = jnp.concatenate(blocks)
    block_squares = jnp.sum(jnp.square(blocks.astype(F32)), axis=2)

    def message(pick):
        taken = jnp.einsum("sct,std->scd", pick.astype(BF), blocks, preferred_element_type=F32)
        taken = (taken.reshape(-1, width) * norm_gain).astype(BF)
        square_sum = jnp.where(pick, block_squares[:, None, :], 0.0).sum(axis=2).reshape(-1)
        high = lax.reduce_precision(square_sum, exponent_bits=8, mantissa_bits=7)
        carried = jnp.stack([high, square_sum - high]).astype(BF).reshape(-1, width)
        return jnp.concatenate([taken, jnp.pad(carried, ((0, -carried.shape[0] % 8), (0, 0)))])

    own_rows, other_rows = message(picks[0]), message(picks[1])

    def chips_met(own, for_next):
        from_up = sent(for_next, "tp", -2)
        from_down = sent(for_next, "tp", 2)
        far = sent(own, "tp", 4)
        seen = [own, from_up, from_down, far]
        return seen + [swapped_between(b, "tp", 1) for b in seen]

    def rows_of(w, at, size):
        return jnp.concatenate([lax.dynamic_slice_in_dim(w, i * size, size, 0) for i in at], axis=0)

    count = ep * capacity
    extra = 2 * count // width
    beside = [own_rows, sent(other_rows, "tp", -2), sent(other_rows, "tp", 2)]
    beside = lax.optimization_barrier(beside)
    across = [sent(beside[0], "tp", 4)]

    def met_rows(blocks_met, weights):
        features = jnp.concatenate(
            [b for met in blocks_met for b in (met, swapped_between(met, "tp", 1))], axis=1
        )
        carried = features[count : count + extra].astype(F32).reshape(extra, -1, width).sum(axis=1)
        return jnp.dot(features, weights, preferred_element_type=F32), carried.reshape(2, count).sum(axis=0)

    both, squares = met_rows(beside, gate_up[0])
    both, across = lax.optimization_barrier((both, across))
    both_far, squares_far = met_rows(across, gate_up[1])
    both, squares = both + both_far, squares + squares_far
    both = both[:count]
    both = both * lax.rsqrt(squares / (width * tp) + EPSILON)[:, None]
    gate_val, up_val = both[:, : 2 * units], both[:, 2 * units :]
    hidden = (jax.nn.silu(gate_val) * up_val).astype(BF)

    met = chips_met(hidden, hidden)
    mine_hidden = jnp.concatenate([met[0], met[3], met[4], met[7]], axis=1)
    other_hidden = jnp.concatenate([met[1], met[2], met[5], met[6]], axis=1)

    def slices_at(c, k):
        return [2 * c + k, (2 * (c + 1 - 2 * k) + k) % tp]

    own_order = [i for k in (core, 1 - core) for c in (chip, chip + 2) for i in slices_at(c, k)]
    other_order = [i for k in (core, 1 - core) for c in (chip + 1, chip - 1) for i in slices_at(c, k)]
    own_down = rows_of(lax.dynamic_index_in_dim(down_weight, mine, 0, keepdims=False), [i % tp for i in own_order], units)
    other_down = rows_of(lax.dynamic_index_in_dim(down_weight, other, 0, keepdims=False), [i % tp for i in other_order], units)
    own_out = jnp.dot(mine_hidden, own_down, preferred_element_type=F32)
    other_out = jnp.dot(other_hidden, other_down, preferred_element_type=F32)

    def back(k, out):
        scaled = (out.reshape(ep, capacity, width) * row_gates[k][:, :, None]).astype(BF)
        return jnp.einsum("sct,scd->std", picks[k].astype(BF), scaled, preferred_element_type=F32)

    partial = (back(0, own_out) + back(1, other_out)).astype(BF)
    return (residual.astype(F32) + summed(partial)).astype(BF)


def solution(mesh):
    return jax.shard_map(
        shards,
        mesh=mesh,
        in_specs=(
            P(("rep", "ep"), "tp"),
            P(("rep", "ep"), "tp"),
            P(("rep", "ep"), None),
            P(("rep", "ep"), None),
            P(("rep", "ep")),
            P("tp", "ep"),
            P("tp"),
            P(("rep", "ep"), None),
            P(("rep", "ep"), None),
            P("ep", None, "tp"),
            P("ep", None, "tp"),
            P("ep", None, "tp"),
        ),
        out_specs=P(("rep", "ep"), "tp"),
        check_vma=False,
    )
```
